32 devices in a mesh: img: 4 (over y, x), seq: 8 (over z, core).
Axes of the slice: x: 2, y: 2, z: 4, core: 2. Of those that a mesh axis runs over, the one named last changes fastest.
Arguments:
- image_query: bfloat16 [4, 1024, 1280], P('img', 'seq'), may hold values from -7 to 7
- image_key: bfloat16 [4, 1024, 1280], P('img', 'seq'), may hold values from -7 to 7
- image_value: bfloat16 [4, 1024, 1280], P('img', 'seq'), may hold values from -3 to 3
- image_output: bfloat16 [4, 1024, 1280], P('img', 'seq'), may hold values from -0.875 to 0.875
- output_grad: bfloat16 [4, 1024, 2432], P('img', 'seq'), may hold values from -48 to 48
- image_logsum: float32 [4, 1024, 20], P('img', 'seq'), may hold values from 8 to 9
- text_query: bfloat16 [4, 333, 1280], P('img'), may hold values from -7 to 7
- text_key: bfloat16 [4, 333, 1280], P('img'), may hold values from -7 to 7
- text_value: bfloat16 [4, 333, 1280], P('img'), may hold values from -3 to 3
- text_output: bfloat16 [4, 333, 1280], P('img'), may hold values from -0.875 to 0.875
- text_grad: bfloat16 [4, 333, 1280], P('img'), may hold values from -48 to 48
- text_logsum: float32 [4, 333, 20], P('img'), may hold values from 8 to 9
- out_weight: bfloat16 [2432, 1280], replicated, may hold values from -0.125 to 0.125
Outputs:
- query_grad: bfloat16 [4, 1024, 1280], P('img', 'seq')
- key_grad: bfloat16 [4, 1024, 1280], P('img', 'seq')
- value_grad: bfloat16 [4, 1024, 1280], P('img', 'seq')
- text_query_grad: bfloat16 [4, 333, 1280], P('img')
- text_key_grad: bfloat16 [4, 333, 1280], P('img')
- text_value_grad: bfloat16 [4, 333, 1280], P('img')
- weight_grad: float32 [2432, 1280], P('seq')
The draws below stay inside these ranges and needn't reach their ends.
All inputs are finite; a program needn't handle non-finite values.
Results may differ from the reference program's by a relative error of at most 0.017.
Values may be sent and summed in bfloat16 or wider, within the bound.
A program may use at most 192 MiB of HBM per device.

```python
import jax
import jax.numpy as jnp
from jax import lax

D = 2432
HEADS = 20
TXT = 333
TOK_DEV = 128
HD = 1280
S = 1024
IMAGES = 4
N_SEQ = 8


def levels(key, extent, cuts, low, largest):
    factor_of, own = 1.0, jax.random.fold_in(key, 6)
    for axis_at, parts in cuts:
        steps = jnp.exp(jax.random.uniform(jax.random.fold_in(own, axis_at), (parts,), jnp.float32, low / len(cuts), largest / len(cuts)))
        factor_of = factor_of * jnp.repeat(steps, extent[axis_at] // parts).reshape([-1 if axis == axis_at else 1 for axis in range(len(extent))])
    return factor_of


def centred(own_key, shape, spread, limit, split=(), dtype=jnp.bfloat16):
    result = jax.random.normal(own_key, shape, jnp.float32) * spread
    if len(split) > 0:
        result = levels(own_key, shape, split, -0.22, 0.18) * result
    return jnp.clip(result, min=-limit, max=limit).astype(dtype)


def setup_inputs(seed: int = 0) -> dict:
    keys = jax.random.split(jax.random.key(seed), 14)
    return {
        "image_query": centred(keys[0], (IMAGES, S, HD), 1.1, 7.0, ((0, 4), (1, 8))),
        "image_key": centred(keys[1], (IMAGES, S, HD), 1.1, 7.0, ((0, 4), (1, 8))),
        "image_value": centred(keys[2], (IMAGES, S, HD), 0.5, 3.0, ((0, 4), (1, 8))),
        "image_output": centred(keys[3], (IMAGES, S, HD), 0.15, 0.875, ((0, 4), (1, 8))),
        "output_grad": centred(keys[4], (IMAGES, S, D), 8.0, 48.0, ((0, 4), (1, 8))),
        "image_logsum": jnp.clip(8.0 + 1.0 * jax.random.uniform(keys[5], (IMAGES, S, HEADS), jnp.float32) ** levels(keys[5], (IMAGES, S, HEADS), ((0, 4), (1, 8)), -0.2, 0.2), 8.0, 9.0),
        "text_query": centred(keys[6], (IMAGES, TXT, HD), 1.1, 7.0, ((0, 4),)),
        "text_key": centred(keys[7], (IMAGES, TXT, HD), 1.1, 7.0, ((0, 4),)),
        "text_value": centred(keys[8], (IMAGES, TXT, HD), 0.5, 3.0, ((0, 4),)),
        "text_output": centred(keys[9], (IMAGES, TXT, HD), 0.15, 0.875, ((0, 4),)),
        "text_grad": centred(keys[10], (IMAGES, TXT, HD), 8.0, 48.0, ((0, 4),)),
        "text_logsum": jnp.clip(8.0 + 1.0 * jax.random.uniform(keys[11], (IMAGES, TXT, HEADS), jnp.float32) ** levels(keys[11], (IMAGES, TXT, HEADS), ((0, 4),), -0.2, 0.2), 8.0, 9.0),
        "out_weight": centred(keys[12], (D, HD), D ** -0.5, 0.125),
    }


def row_dot(grads_out, outputs, head_count):
    product = grads_out.astype(jnp.float32) * outputs.astype(jnp.float32)
    return product.reshape(product.shape[0], head_count, -1).sum(axis=-1)


def pair_grads(queries, grads_out, log_sum, row_dots, key_rows, value_rows):
    head_count = log_sum.shape[1]
    query_count = queries.shape[0]
    key_count = key_rows.shape[0]
    head_width = queries.shape[1] // head_count
    scaling = head_width ** -0.5
    query_heads = queries.astype(jnp.float32).reshape(query_count, head_count, head_width)
    grad_heads = grads_out.astype(jnp.float32).reshape(query_count, head_count, head_width)
    key_heads = key_rows.astype(jnp.float32).reshape(key_count, head_count, head_width)
    value_heads = value_rows.astype(jnp.float32).reshape(key_count, head_count, head_width)
    scores = jnp.einsum("qhe,khe->hqk", query_heads, key_heads) * scaling
    weights = jnp.exp(scores - log_sum.T[:, :, None])
    grad_weights = jnp.einsum("qhe,khe->hqk", grad_heads, value_heads)
    grad_scores = weights * (grad_weights - row_dots.T[:, :, None])
    weights_low = lax.optimization_barrier(weights.astype(jnp.bfloat16)).astype(jnp.float32)
    scores_low = lax.optimization_barrier(grad_scores.astype(jnp.bfloat16)).astype(jnp.float32)
    query_part = jnp.einsum("hqk,khe->qhe", scores_low, key_heads) * scaling
    key_part = jnp.einsum("hqk,qhe->khe", scores_low, query_heads) * scaling
    value_part = jnp.einsum("hqk,qhe->khe", weights_low, grad_heads)
    return (query_part.reshape(query_count, -1), key_part.reshape(key_count, -1),
            value_part.reshape(key_count, -1))


def reference(image_query, image_key, image_value, image_output, output_grad, image_logsum,
              text_query, text_key, text_value, text_output, text_grad, text_logsum, out_weight):
    head_count = image_logsum.shape[-1]

    def one_image(inputs):
        (queries, key_rows, value_rows, outputs, upstream, log_sum,
         text_queries, text_keys, text_values, text_outs, text_dout, text_lsum) = inputs
        image_dout = jnp.dot(upstream, out_weight, preferred_element_type=jnp.float32).astype(jnp.bfloat16)
        image_dots = row_dot(image_dout, outputs, head_count)
        text_dots = row_dot(text_dout, text_outs, head_count)
        all_keys = jnp.concatenate([key_rows, text_keys], axis=0)
        all_values = jnp.concatenate([value_rows, text_values], axis=0)
        feature = queries.shape[1]
        length = queries.shape[0]

        def query_block(running, section):
            block_query, block_dout, block_lsum, block_dots = section
            query_part, key_part, value_part = pair_grads(block_query, block_dout, block_lsum, block_dots,
                                                          all_keys, all_values)
            return (running[0] + key_part, running[1] + value_part), query_part

        zeros_grad = jnp.zeros(all_keys.shape, jnp.float32)
        sections = (queries.reshape(N_SEQ, TOK_DEV, feature), image_dout.reshape(N_SEQ, TOK_DEV, feature),
                    log_sum.reshape(N_SEQ, TOK_DEV, head_count), image_dots.reshape(N_SEQ, TOK_DEV, head_count))
        (key_total, value_total), query_blocks = lax.scan(query_block, (zeros_grad, zeros_grad), sections)
        text_qpart, text_kpart, text_vpart = pair_grads(text_queries, text_dout, text_lsum, text_dots,
                                                        all_keys, all_values)
        key_total = key_total + text_kpart
        value_total = value_total + text_vpart

        def weight_block(running, section):
            block_grad, block_out = section
            term = jnp.dot(block_grad.T, block_out, preferred_element_type=jnp.float32)
            return running + lax.optimization_barrier(term.astype(jnp.bfloat16)).astype(jnp.float32), None

        weight_total, ignored = lax.scan(
            weight_block, jnp.zeros((upstream.shape[1], feature), jnp.float32),
            (upstream.reshape(N_SEQ, TOK_DEV, upstream.shape[1]), outputs.reshape(N_SEQ, TOK_DEV, feature)))
        return (query_blocks.reshape(length, feature).astype(jnp.bfloat16),
                key_total[:length].astype(jnp.bfloat16), value_total[:length].astype(jnp.bfloat16),
                text_qpart.astype(jnp.bfloat16), key_total[length:].astype(jnp.bfloat16),
                value_total[length:].astype(jnp.bfloat16), weight_total)

    results = lax.map(one_image, (image_query, image_key, image_value, image_output, output_grad, image_logsum,
                                  text_query, text_key, text_value, text_output, text_grad, text_logsum))
    return (results[0], results[1], results[2], results[3], results[4], results[5],
            jnp.sum(results[6], axis=0))
```

```python
import functools

import jax
import jax.numpy as jnp
from jax import lax
from jax.experimental import pallas as pl
from jax.experimental.pallas import tpu as pltpu
from jax.sharding import PartitionSpec as P

STATS = 128
PARTS = 3
NT = (((1,), (1,)), ((), ()))
TN = (((0,), (0,)), ((), ()))


def attention_kernel(heads, width, key_block, x_ref, out_ref, q_s, k_s, v_s, g_s, dk_s, dv_s, dq_s):
    total = x_ref.shape[0]
    span = heads * width
    aug = q_s.shape[1] - width
    scaling = width ** (-0.5)
    stats = x_ref[:, 4 * span : 4 * span + aug]
    lane = lax.broadcasted_iota(jnp.int32, (total, aug), 1)
    for head in range(heads):
        base = head * 2 * PARTS

        def ones(start):
            inside = (lane >= start) & (lane < start + PARTS)
            return jnp.where(inside, 1.0, 0.0).astype(jnp.bfloat16)

        def part(number):
            start = number * span + head * width
            return x_ref[:, start : start + width]

        q_s[...] = jnp.concatenate([part(0), stats], axis=1)
        k_s[...] = jnp.concatenate([part(1), ones(base)], axis=1)
        v_s[...] = jnp.concatenate([part(2), ones(base + PARTS)], axis=1)
        g_s[...] = jnp.concatenate([part(3), stats], axis=1)
        dq_s[...] = jnp.zeros_like(dq_s)

        @pl.loop(0, total // key_block)
        def _(step):
            rows = pl.ds(pl.multiple_of(step * key_block, key_block), key_block)
            keys = k_s[rows, :]
            scores = lax.dot_general(keys, q_s[...], NT, preferred_element_type=jnp.float32)
            weights = jnp.exp(scores)
            grads = lax.dot_general(v_s[rows, :], g_s[...], NT, preferred_element_type=jnp.float32)
            low = (weights * grads).astype(jnp.bfloat16)
            dv_s[rows, :] = jnp.dot(
                weights.astype(jnp.bfloat16), g_s[...], preferred_element_type=jnp.float32
            ).astype(jnp.bfloat16)
            dk_s[rows, :] = jnp.dot(low, q_s[...], preferred_element_type=jnp.float32).astype(
                jnp.bfloat16
            )
            dq_s[...] += lax.dot_general(keys, low, TN, preferred_element_type=jnp.float32)

        def put(number, value):
            start = number * span + head * width
            out_ref[:, start : start + width] = value[:, :width]

        put(0, (dq_s[...].T * scaling).astype(jnp.bfloat16))
        put(1, dk_s[...])
        put(2, dv_s[...])


def attention(x, heads, width):
    total = x.shape[0]
    key_block = total // 8
    depth = 2 * width
    return pl.pallas_call(
        functools.partial(attention_kernel, heads, width, key_block),
        out_shape=jax.ShapeDtypeStruct((total, 3 * heads * width), jnp.bfloat16),
        in_specs=[pl.BlockSpec(memory_space=pltpu.VMEM)],
        out_specs=pl.BlockSpec(memory_space=pltpu.VMEM),
        scratch_shapes=[pltpu.VMEM((total, depth), jnp.bfloat16)] * 6
        + [pltpu.VMEM((depth, total), jnp.float32)],
        compiler_params=pltpu.CompilerParams(vmem_limit_bytes=48 << 20),
        cost_estimate=pl.CostEstimate(
            flops=20 * heads * total * total * width,
            bytes_accessed=14 * total * heads * width,
            transcendentals=heads * total * total,
        ),
    )(x)


def row_dot(grads_out, outputs, head_count):
    product = grads_out.astype(jnp.float32) * outputs.astype(jnp.float32)
    return product.reshape(product.shape[0], head_count, -1).sum(axis=-1)


def split_low(value):
    terms = []
    for _ in range(PARTS):
        term = lax.reduce_precision(value, 8, 7)
        terms.append(term.astype(jnp.bfloat16))
        value = value - term
    return jnp.stack(terms, axis=-1)


def add_low(terms):
    return sum(term.astype(jnp.float32) for term in terms).astype(jnp.bfloat16)


def scatter_sum(pieces, axis, stride, place):
    size = lax.axis_size(axis)
    count = pieces.shape[0]
    terms = [lax.dynamic_index_in_dim(pieces, place, axis=0, keepdims=False)]
    for shift in range(1, count):
        pairs = [
            (source, (source + shift * stride) % (count * stride) if stride * count == size else source ^ 1)
            for source in range(size)
        ]
        outgoing = lax.dynamic_index_in_dim(
            pieces, lax.rem(place + shift, count), axis=0, keepdims=False
        )
        terms.append(lax.ppermute(outgoing, axis, pairs))
    return add_low(terms)


def reduce_term(term, peers):
    images = lax.axis_size("img")
    me = lax.axis_index("seq")
    piece = term.shape[0] // (peers * images)
    blocks = term.reshape(peers // 2, 2, images, piece, term.shape[1])
    blocks = scatter_sum(blocks.transpose(1, 0, 2, 3, 4), "seq", 1, lax.rem(me, 2))
    blocks = scatter_sum(blocks.transpose(1, 0, 2, 3), "img", 1, lax.axis_index("img"))
    return scatter_sum(blocks, "seq", 2, me // 2)


def shards(
    image_query,
    image_key,
    image_value,
    image_output,
    output_grad,
    image_logsum,
    text_query,
    text_key,
    text_value,
    text_output,
    text_grad,
    text_logsum,
    out_weight,
):
    peers = lax.axis_size("seq")
    me = lax.axis_index("seq")
    head_count = image_logsum.shape[-1]
    rows, feature = image_query.shape[1:]
    text_rows = text_query.shape[1]
    width = feature // head_count
    heads = -(-head_count // peers)
    span = heads * width
    scaling = width ** (-0.5)

    weight_term = lax.dot_general(
        output_grad[0], image_output[0], TN, preferred_element_type=jnp.float32
    ).astype(jnp.bfloat16)

    upstream, weight_term = lax.optimization_barrier((output_grad[0], weight_term))
    weight_sum = reduce_term(weight_term, peers)
    image_dout = jnp.dot(
        upstream, out_weight, preferred_element_type=jnp.float32
    ).astype(jnp.bfloat16)

    def widen(array, columns):
        return jnp.pad(array, ((0, 0), (0, columns - array.shape[1])))

    def pack(query, key, value, grad, output, log_sum, groups):
        count = query.shape[0]
        dots = row_dot(grad, output, log_sum.shape[1])
        stats = jnp.stack([-log_sum, -dots], axis=-1)
        terms = split_low(stats).reshape(count, groups, heads * 2 * PARTS)
        terms = jnp.pad(terms, ((0, 0), (0, 0), (0, STATS - terms.shape[-1])))
        scaled = query * jnp.asarray(scaling, query.dtype)
        parts = [part.reshape(count, groups, span) for part in (scaled, key, value, grad)]
        return jnp.concatenate([*parts, terms], axis=-1)

    def mine(array, columns):
        padded = widen(array, peers * columns)
        return lax.dynamic_slice_in_dim(padded, me * columns, columns, axis=1)

    image_arrays = (image_query[0], image_key[0], image_value[0], image_dout, image_output[0])
    image_pack = pack(
        *(widen(array, peers * span) for array in image_arrays),
        widen(image_logsum[0], peers * heads),
        peers,
    )
    image_all = lax.all_to_all(image_pack.transpose(1, 0, 2), "seq", 0, 0)
    text_arrays = (text_query[0], text_key[0], text_value[0], text_grad[0], text_output[0])
    text_mine = pack(
        *(mine(array, span) for array in text_arrays), mine(text_logsum[0], heads), 1
    )[:, 0]

    tokens = peers * rows + text_rows
    total = -(-tokens // 128) * 128
    x = jnp.concatenate([image_all.reshape(peers * rows, -1), text_mine], axis=0)
    x = jnp.pad(x, ((0, total - tokens), (0, 0)))
    grads = attention(x, heads, width)

    image_back = lax.all_to_all(
        grads[: peers * rows].reshape(peers, rows, 3 * span), "seq", 0, 0
    )
    text_back = lax.all_gather(grads[peers * rows : tokens], "seq", axis=0)
    weight_grad = lax.all_gather(weight_sum, "img", axis=0, tiled=True).astype(jnp.float32)

    def finish(back):
        results = []
        for number in range(3):
            piece = back[:, :, number * span : (number + 1) * span].transpose(1, 0, 2)
            results.append(piece.reshape(back.shape[1], peers * span)[None, :, :feature])
        return results

    return (*finish(image_back), *finish(text_back), weight_grad)


def solution(mesh):
    token = P("img", "seq", None)
    text = P("img", None, None)
    return jax.shard_map(
        shards,
        mesh=mesh,
        in_specs=(token,) * 6 + (text,) * 6 + (P(),),
        out_specs=(token,) * 3 + (text,) * 3 + (P("seq", None),),
        check_vma=False,
    )
```
